32 devices in a mesh: row: 8 (over y, x, core), col: 4 (over z).
Axes of the slice: x: 2, y: 2, z: 4, core: 2. Of those that a mesh axis runs over, the one named last changes fastest.
Arguments:
- design: bfloat16 [4096, 6144], P(('row', 'col')), may hold values from -0.09375 to 0.09375
- observations: float32 [4096], P(('row', 'col')), may hold values from -6 to 6
- gaps: int32 [4096], P(('row', 'col')), may hold values 0 or 1
- noise_var: float32 [4096], P(('row', 'col')), may hold values from 0.25 to 4
- arc_lengths: int32 [32, 4], P(('row', 'col')), may hold values from 1 to 64, 128 in all within a row
- arc_amp: float32 [32, 4], P(('row', 'col')), may hold values from 0.2 to 2
- arc_decay: float32 [32, 4], P(('row', 'col')), may hold values from 0.3 to 0.95
- plan: int32 [32], P(('row', 'col')), may hold values from 0 to 31, each once
- tile_map: int32 [48], replicated, may hold values from 0 to 47, each once
Outputs:
- gram: float32 [6144, 6144], P('row', 'col')
- normal_rhs: float32 [6144], P('row')
- balanced_obs: float32 [32, 128], P(('row', 'col'))
The draws below stay inside these ranges and needn't reach their ends.
Inputs may be any that keep to these rules, and one draw needn't show every extreme that they name: `plan`: a permutation of the blocks. `tile_map`: a permutation of the tiles. `arc_lengths`: each block's arc lengths sum to 128; some arc has 64 rows.
All inputs are finite; a program needn't handle non-finite values. No bound on the sum of `gaps` on one device may be relied on, other than what follows from the above.
Results may differ from the reference program's by a relative error of at most 0.004.
Values may be sent and summed in bfloat16 or wider, within the bound.
A program may use at most 192 MiB of HBM per device.

```python
import math
import jax
import jax.numpy as jnp
import numpy as np
from jax import lax

U = 6144
TB = 128
SB = 128
ARCS = 4
MAXARC = 64
BLOCKS = 32
ROWS = 4096


def set_ends(values, rng, low, high):
    longest = values.shape.index(max(values.shape))
    spots = []
    for shift in (0, 1):
        where = [jax.random.randint(jax.random.fold_in(rng, axis), (), 0, length) for axis, length in enumerate(values.shape)]
        where[longest] = (where[longest] + shift) % values.shape[longest]
        spots.append(tuple(where))
    return values.at[spots[0]].set(low).at[spots[1]].set(high)


def level_of(rng, shape, cuts, smallest, high):
    factor_of, own = 1.0, jax.random.fold_in(rng, 6)
    for dim, blocks in cuts:
        draws = jnp.exp(jax.random.uniform(jax.random.fold_in(own, dim), (blocks,), jnp.float32, smallest / len(cuts), high / len(cuts)))
        factor_of = factor_of * jnp.repeat(draws, shape[dim] // blocks).reshape([-1 if axis == dim else 1 for axis in range(len(shape))])
    return factor_of


def profile(count, total, reach, slope):
    weights = [(1 << 20) // math.isqrt(grade ** slope) + 1 for grade in range(2, count + 1)]
    rest, given = total - reach - (count - 1), [1] * (count - 1)
    while rest > 0:
        candidates = [i for i in range(count - 1) if given[i] < reach]
        mass, budget = sum([weights[i] for i in candidates]), rest
        for i in candidates:
            extra = min(reach - given[i], max(1, budget * weights[i] // mass), rest)
            given[i] = given[i] + extra
            rest = rest - extra
    return np.array([reach] + given)


def uneven_parts(own_key, count, total, bound, skew):
    if count == 2:
        one = jax.random.randint(own_key, (), max(1, total - bound), min(bound, total - 1) + 1)
        return jnp.stack([one, total - one])
    sizes = jnp.asarray(profile(count, total, bound, skew), jnp.int32)
    pairs = (count - 1) // 2
    giver, receiver = sizes[1:1 + 2 * pairs:2], sizes[2:2 + 2 * pairs:2]
    room = jnp.minimum(giver - 1, bound - receiver)
    shifted = jax.random.randint(jax.random.fold_in(own_key, 1), (pairs,), 0, 1 << 20) % (room + 1)
    sizes = sizes.at[1:1 + 2 * pairs:2].set(giver - shifted).at[2:2 + 2 * pairs:2].set(receiver + shifted)
    return sizes[jax.random.permutation(jax.random.fold_in(own_key, 2), count)]


def gaussian(key, dims, deviation, most, split=(), held_as=jnp.bfloat16):
    array = jax.random.normal(key, dims, jnp.float32) * deviation
    if len(split) > 0:
        array = level_of(key, dims, split, -0.22, 0.18) * array
    return jnp.clip(array, min=-most, max=most).astype(held_as)


def setup_inputs(seed: int = 0) -> dict:
    key_list = jax.random.split(jax.random.key(seed), 10)
    return {
        "design": gaussian(key_list[0], (ROWS, U), (ROWS ** -0.5), 0.09375, ((0, 32),)),
        "observations": gaussian(key_list[1], (ROWS,), 1.0, 6.0, ((0, 32),), jnp.float32),
        "gaps": set_ends((jax.random.randint(key_list[2], (ROWS,), 0, 8) < 7).astype(jnp.int32), jax.random.fold_in(key_list[2], 1), 0, 1),
        "noise_var": jnp.clip(jnp.exp(math.log(4.0) - 2.7725887 * jax.random.uniform(key_list[3], (ROWS,), jnp.float32) ** level_of(key_list[3], (ROWS,), ((0, 32),), -0.2, 0.2)), 0.25, 4.0),
        "arc_lengths": jax.vmap(lambda own: uneven_parts(own, ARCS, SB, MAXARC, 2))(jax.random.split(key_list[4], BLOCKS)).reshape((BLOCKS, ARCS)).astype(jnp.int32),
        "arc_amp": jnp.clip(jnp.exp(math.log(2.0) - 2.3025851 * jax.random.uniform(key_list[5], (BLOCKS, ARCS), jnp.float32) ** level_of(key_list[5], (BLOCKS, ARCS), ((0, 32),), -0.2, 0.2)), 0.2, 2.0),
        "arc_decay": jnp.clip(0.3 + 0.65 * jax.random.uniform(key_list[6], (BLOCKS, ARCS), jnp.float32) ** level_of(key_list[6], (BLOCKS, ARCS), ((0, 32),), -0.2, 0.2), 0.3, 0.95),
        "plan": jax.random.permutation(key_list[7], BLOCKS).astype(jnp.int32),
        "tile_map": jax.random.permutation(key_list[8], U // TB).astype(jnp.int32),
    }


def whiten(block, obs_rows, live_rows, noise_rows, lengths, amplitude, decay):
    block_rows = block.shape[0]
    arc_count = lengths.shape[0]
    position = jnp.arange(block_rows, dtype=jnp.int32)
    arc_ends = jnp.cumsum(lengths).astype(jnp.int32)
    arc_id = jnp.sum((arc_ends[None, :] <= position[:, None]).astype(jnp.int32), axis=1)
    member = (arc_id[:, None] == jnp.arange(arc_count, dtype=jnp.int32)[None, :]).astype(jnp.float32)
    row_amp = jnp.sum(member * amplitude[None, :], axis=1)
    row_rate = jnp.sum(member * jnp.log(decay)[None, :], axis=1)
    same_arc = (arc_id[:, None] == arc_id[None, :]).astype(jnp.float32)
    row_lag = jnp.abs(position[:, None] - position[None, :]).astype(jnp.float32)
    kernel = row_amp[:, None] * jnp.exp(row_lag * row_rate[:, None]) * same_arc * live_rows[:, None] * live_rows[None, :]
    covariance = kernel + jnp.diag(noise_rows)
    factor = jnp.linalg.cholesky(covariance)
    solved = lax.linalg.triangular_solve(factor, block.astype(jnp.float32) * live_rows[:, None], left_side=True, lower=True)
    solved_obs = lax.linalg.triangular_solve(factor, (obs_rows * live_rows)[:, None], left_side=True, lower=True)
    return (solved.astype(jnp.bfloat16), solved_obs[:, 0])

def reference(design, observations, gaps, noise_var, arc_lengths, arc_amp, arc_decay, plan, tile_map):
    block_count = arc_lengths.shape[0]
    block_rows = design.shape[0] // block_count
    columns = design.shape[1]
    tile_count = tile_map.shape[0]
    tile_size = columns // tile_count
    live_rows = gaps.astype(jnp.float32)

    def one_block(inputs):
        return whiten(*inputs)
    white, white_obs = lax.map(one_block, (design.reshape(block_count, block_rows, columns), observations.reshape(block_count, block_rows), live_rows.reshape(block_count, block_rows), noise_var.reshape(block_count, block_rows), arc_lengths, arc_amp, arc_decay))
    slotted = white.reshape(-1, tile_count, tile_size)[:, tile_map, :].reshape(-1, columns)
    widened = slotted.astype(jnp.float32)
    gram = jnp.dot(widened.T, widened, precision=lax.Precision.HIGHEST)
    obs_half = white_obs.reshape(-1).astype(jnp.bfloat16)
    normal_rhs = jnp.dot(obs_half.astype(jnp.float32), slotted.astype(jnp.float32), preferred_element_type=jnp.float32)
    balanced_obs = white_obs[plan]
    return (gram, normal_rhs, balanced_obs)
```

```python
import functools

import jax
import jax.numpy as jnp
from jax import lax
from jax.experimental import pallas as pl
from jax.experimental.pallas import tpu as pltpu
from jax.sharding import PartitionSpec as P

MESH = pl.DeviceIdType.MESH
EXTRA = 16


def by_row(vector, rows):
    return jnp.transpose(jnp.broadcast_to(vector, (rows, vector.shape[1])))


def whiten_kernel(
    arcs, tile_map, lengths, amps, decays, design, obs, gaps, noise,
    white, white_t, live_m, noise_m, phi_m, amp_m, start_m, inno_m, var_m, parts,
):
    rows = design.shape[0]
    slots_z = white.shape[0] * white.shape[1] * white.shape[3] // rows
    half_tiles = white.shape[3] // rows
    row_tiles = (white_t.shape[1] - EXTRA) // rows
    live_row = gaps[...].astype(jnp.float32)
    live_m[...] = by_row(live_row, rows)
    noise_m[...] = by_row(noise[...], rows)
    position = lax.broadcasted_iota(jnp.int32, (rows, rows), 0)
    lane = lax.broadcasted_iota(jnp.int32, (rows, rows), 1)
    phi = jnp.zeros((rows, rows), jnp.float32)
    amp = jnp.zeros((rows, rows), jnp.float32)
    first = jnp.zeros((rows, rows), jnp.float32)
    begin = jnp.int32(0)
    for a in range(arcs):
        end = begin + lengths[0, a]
        inside = jnp.logical_and(position >= begin, position < end)
        phi = jnp.where(inside, decays[0, a], phi)
        amp = jnp.where(inside, amps[0, a], amp)
        first = jnp.where(jnp.logical_and(inside, position == begin), 1.0, first)
        begin = end
    phi_m[...] = jnp.where(first > 0.5, 0.0, phi)
    amp_m[...] = jnp.where(first > 0.5, amp, amp * (1.0 - phi * phi))
    start_m[...] = jnp.where(position == lane, 1.0, 0.0)

    def step(k, carry):
        state, spread = carry
        at = pl.ds(k, 1)
        rate, live, floor = phi_m[at, :], live_m[at, :], noise_m[at, :]
        state = rate * state
        spread = rate * rate * spread + amp_m[at, :]
        var = spread * live + floor
        ratio = 1.0 / var
        inno = live * (start_m[at, :] - state)
        inno_m[at, :] = inno
        var_m[at, :] = var
        return state + (spread * live * ratio) * inno, spread * floor * ratio

    zero = jnp.zeros((1, rows), jnp.float32)
    lax.fori_loop(0, rows, step, (zero, zero), unroll=8)
    inverse = inno_m[...] / jnp.sqrt(var_m[...])
    high = inverse.astype(jnp.bfloat16)
    rest = inverse - high.astype(jnp.float32)
    mid = rest.astype(jnp.bfloat16)
    parts[0] = high
    parts[1] = mid
    parts[2] = (rest - mid.astype(jnp.float32)).astype(jnp.bfloat16)

    def slot(s, _):
        column = pl.multiple_of(tile_map[s] * rows, rows)
        tile = design[:, pl.ds(column, rows)]
        solved = jnp.dot(parts[2], tile, preferred_element_type=jnp.float32)
        solved += jnp.dot(parts[1], tile, preferred_element_type=jnp.float32)
        solved += jnp.dot(parts[0], tile, preferred_element_type=jnp.float32)
        place = lax.rem(s, half_tiles)
        piece = s // half_tiles
        white[piece // 2, lax.rem(piece, 2), :, pl.ds(pl.multiple_of(place * rows, rows), rows)] = (
            solved.astype(jnp.bfloat16)
        )
        low = pl.multiple_of(lax.rem(s, row_tiles) * rows, rows)
        white_t[s // row_tiles, pl.ds(low, rows), :] = jnp.transpose(solved).astype(jnp.bfloat16)
        return 0

    lax.fori_loop(0, slots_z, slot, 0, unroll=4)
    obs_m = by_row(obs[...], rows)
    solved_obs = jnp.sum(jnp.transpose(inverse) * obs_m, axis=0, keepdims=True)
    o_high = solved_obs.astype(jnp.bfloat16).astype(jnp.float32)
    o_rest = solved_obs - o_high
    o_mid = o_rest.astype(jnp.bfloat16).astype(jnp.float32)
    which = lax.broadcasted_iota(jnp.int32, (EXTRA, rows), 0)
    packed = jnp.where(which == 0, o_high, 0.0)
    packed = jnp.where(which == 1, o_mid, packed)
    packed = jnp.where(which == 2, o_rest - o_mid, packed).astype(jnp.bfloat16)
    for r in range(white_t.shape[0]):
        white_t[r, row_tiles * rows :, :] = packed


def gram_kernel(R, C, w, wt, gram, rhs, obs, rp, cp, *sems):
    (r1s, r1r, ups, upr, dns, dnr, c1s, c1r, c2s, c2r, c3s, c3r) = sems
    r, z = lax.axis_index("row"), lax.axis_index("col")
    bits = [1 << i for i in range(1, (R - 1).bit_length())]
    orders = (bits, bits[::-1])
    M = gram.shape[0]

    def flip(mask):
        out = r
        bit = 1
        while bit <= mask:
            if mask & bit:
                out = out + bit - 2 * bit * lax.rem(r // bit, 2)
            bit *= 2
        return out

    zof = lambda d: lax.rem(z + (d % C), C)
    blk = lambda mask, d: flip(mask) * C + zof(d)
    own = r * C + z

    barrier = pltpu.get_barrier_semaphore()
    for mask in range(1, R):
        pl.semaphore_signal(barrier, inc=1, device_id=(flip(mask), z), device_id_type=MESH)
    for d in range(1, C):
        pl.semaphore_signal(barrier, inc=1, device_id=(r, zof(d)), device_id_type=MESH)
    pl.semaphore_wait(barrier, R - 1 + C - 1)

    sent = []

    def send(src, dst, ss, rs, to):
        copy = pltpu.make_async_remote_copy(
            src_ref=src, dst_ref=dst, send_sem=ss, recv_sem=rs, device_id=to, device_id_type=MESH
        )
        copy.start()
        sent.append(copy)

    def arrived(dst, ss, rs):
        pltpu.make_async_remote_copy(
            src_ref=dst, dst_ref=dst, send_sem=ss, recv_sem=rs, device_id=(r, z), device_id_type=MESH
        ).wait_recv()

    def reach(d):
        long, short = C // 2, C - 1 - C // 2
        return (long, short) if d % 2 == 0 else (short, long)

    def ring(d, hop, way):
        at = blk(d, -hop if way > 0 else hop)
        src = wt.at[r] if d == 0 and hop == 0 else rp.at[at]
        ss, rs = (ups, upr) if way > 0 else (dns, dnr)
        send(src, rp.at[at], ss.at[d, hop], rs.at[d, hop], (r, zof(way)))

    def ring_wait(d, hop, way):
        at = blk(d, -(hop + 1) if way > 0 else hop + 1)
        ss, rs = (ups, upr) if way > 0 else (dns, dnr)
        arrived(rp.at[at], ss.at[d, hop], rs.at[d, hop])

    def start_rings(d):
        up, down = reach(d)
        if up > 0:
            ring(d, 0, 1)
        if down > 0:
            ring(d, 0, -1)

    def plane(mask, dz, h, k):
        at = blk(mask, dz)
        bit = orders[h][k]
        src = w.at[z, h] if mask == 0 and dz == 0 else cp.at[at, h]
        i = (mask | bit) // 2
        send(src, cp.at[at, h], c2s.at[h, i, dz], c2r.at[h, i, dz], (flip(bit), z))

    def plane_wait(mask, dz, h):
        i = mask // 2
        arrived(cp.at[blk(mask, dz), h], c2s.at[h, i, dz], c2r.at[h, i, dz])

    def partner(mask, dz):
        at = blk(mask, dz)
        src = w.at[z] if mask == 0 and dz == 0 else cp.at[at]
        send(src, cp.at[at], c3s.at[mask // 2, dz], c3r.at[mask // 2, dz], (flip(1), z))

    def spread(dz):
        for k in range(len(bits)):
            for h in (0, 1):
                plane(0, dz, h, k)
        partner(0, dz)

    zs = sorted(range(C), key=lambda d: (min(d, C - d), d))
    masks = sorted(range(R), key=lambda m: (bin(m >> 1).count("1"), m))
    for d in zs[1:]:
        send(w.at[zof(d)], cp.at[own], c1s.at[d], c1r.at[d], (r, zof(d)))
    for mask in masks[1:]:
        send(wt.at[flip(mask)], rp.at[own], r1s.at[mask], r1r.at[mask], (flip(mask), z))
    spread(0)
    start_rings(0)
    rp[own] = wt[r]
    cp[own] = w[z]
    for i in range(max(R, C)):
        if 0 < i < R:
            mask = masks[i]
            arrived(rp.at[blk(mask, 0)], r1s.at[mask], r1r.at[mask])
            start_rings(mask)
        if 0 < i < C:
            d = zs[i]
            arrived(cp.at[blk(0, -d)], c1s.at[d], c1r.at[d])
            spread((-d) % C)

    ring_jobs = []
    for hop in range(1, C):
        for d in masks:
            up, down = reach(d)
            if hop < up:
                ring_jobs.append((d, hop, 1))
            if hop < down:
                ring_jobs.append((d, hop, -1))
    plane_jobs = []
    even = [m for m in masks if m % 2 == 0]
    for m in even[1:]:
        for dz in zs:
            plane_jobs.append((m, dz))
    done_ring = set()
    for i in range(max(len(ring_jobs), len(plane_jobs))):
        if i < len(plane_jobs):
            m, dz = plane_jobs[i]
            for h in (0, 1):
                plane_wait(m, dz, h)
                last = max(orders[h].index(b) for b in orders[h] if m & b)
                for k in range(last + 1, len(bits)):
                    plane(m, dz, h, k)
            partner(m, dz)
        if i < len(ring_jobs):
            d, hop, way = ring_jobs[i]
            ring_wait(d, hop - 1, way)
            done_ring.add((d, hop - 1, way))
            ring(d, hop, way)

    K = rp.shape[2]
    half = cp.shape[3]
    wide = 256 if half % 256 == 0 else 128
    seen_row, fresh = set(), True
    order = sorted(
        [(m, dz) for m in even for dz in range(C)],
        key=lambda t: (max(bin(t[0]).count("1"), min(t[1], C - t[1])), t[0], t[1]),
    )
    for m, dz in order:
        for d in (m, m | 1):
            if dz != 0:
                up, down = reach(d)
                item = (d, dz - 1, -1) if dz <= down else (d, C - dz - 1, 1)
                if item not in done_ring:
                    ring_wait(*item)
                    done_ring.add(item)
        arrived(cp.at[blk(m | 1, dz)], c3s.at[m // 2, dz], c3r.at[m // 2, dz])
        b0, b1 = blk(m, dz), blk(m | 1, dz)
        left = jnp.concatenate([rp[b0, :M, :], rp[b1, :M, :]], axis=1)
        seen = jnp.concatenate([rp[b0, M:, :], rp[b1, M:, :]], axis=1)
        obs[b0] = rp[b0, M:, :]
        obs[b1] = rp[b1, M:, :]
        side = lax.dot_general(
            seen, left, (((1,), (1,)), ((), ())), preferred_element_type=jnp.float32
        )
        if fresh:
            rhs[...] = side
        else:
            rhs[...] += side

        for h in (0, 1):

            def tile(j, _, h=h, b0=b0, b1=b1, fresh=fresh):
                at = pl.ds(pl.multiple_of(j * wide, wide), wide)
                to = pl.ds(pl.multiple_of(h * half + j * wide, wide), wide)
                lhs = jnp.concatenate([rp[b0, :M, :], rp[b1, :M, :]], axis=1)
                right = jnp.concatenate([cp[b0, h, :, at], cp[b1, h, :, at]], axis=0)
                part = jnp.dot(lhs, right, preferred_element_type=jnp.float32)
                if fresh:
                    gram[:, to] = part
                else:
                    gram[:, to] += part
                return 0

            lax.fori_loop(0, half // wide, tile, 0)
        fresh = False
    for copy in sent:
        copy.wait_send()


def on_device(R, C, design, observations, gaps, noise_var, lengths, amps, decays, plan, tile_map):
    rows, columns = design.shape
    tiles = tile_map.shape[0]
    width = columns // C
    tall = columns // R
    blocks = R * C
    vm = pl.BlockSpec(memory_space=pltpu.VMEM)
    sm = pl.BlockSpec(memory_space=pltpu.SMEM)
    square = pltpu.VMEM((rows, rows), jnp.float32)
    w, wt = pl.pallas_call(
        functools.partial(whiten_kernel, lengths.shape[1]),
        out_shape=(
            jax.ShapeDtypeStruct((C, 2, rows, width // 2), jnp.bfloat16),
            jax.ShapeDtypeStruct((R, tall + EXTRA, rows), jnp.bfloat16),
        ),
        in_specs=[sm, sm, sm, sm, vm, vm, vm, vm],
        out_specs=(vm, vm),
        scratch_shapes=[square] * 7 + [pltpu.VMEM((3, rows, rows), jnp.bfloat16)],
        name="whiten",
    )(
        tile_map, lengths, amps, decays, design,
        observations[None, :], gaps[None, :], noise_var[None, :],
    )
    dma = lambda *shape: pltpu.SemaphoreType.DMA(shape)
    sems = []
    for shape in ((R,), (R, C), (R, C), (C,), (2, R // 2, C), (R // 2, C)):
        sems += [dma(*shape), dma(*shape)]
    gram, rhs, obs = pl.pallas_call(
        functools.partial(gram_kernel, R, C),
        out_shape=(
            jax.ShapeDtypeStruct((tall, width), jnp.float32),
            jax.ShapeDtypeStruct((EXTRA, tall), jnp.float32),
            jax.ShapeDtypeStruct((blocks, EXTRA, rows), jnp.bfloat16),
        ),
        in_specs=[vm, vm],
        out_specs=(vm, vm, vm),
        scratch_shapes=[
            pltpu.VMEM((blocks, tall + EXTRA, rows), jnp.bfloat16),
            pltpu.VMEM((blocks, 2, rows, width // 2), jnp.bfloat16),
        ]
        + sems,
        compiler_params=pltpu.CompilerParams(
            collective_id=0, has_side_effects=True, vmem_limit_bytes=63 * 1024 * 1024
        ),
        name="gram",
    )(w, wt)
    picked = jnp.take(obs, plan, axis=0).astype(jnp.float32)
    balanced = picked[:, 0] + (picked[:, 1] + picked[:, 2])
    return gram, rhs[0], balanced


def solution(mesh):
    both = ("row", "col")
    placed = (
        P(both, None), P(both), P(both), P(both), P(both, None), P(both, None), P(both, None),
        P(both), P(),
    )
    return jax.shard_map(
        functools.partial(on_device, mesh.shape["row"], mesh.shape["col"]),
        mesh=mesh,
        in_specs=placed,
        out_specs=(P("row", "col"), P("row"), P(both, None)),
        check_vma=False,
    )
```

```python
import functools

import jax
import jax.numpy as jnp
from jax import lax
from jax.experimental import pallas as pl
from jax.experimental.pallas import tpu as pltpu
from jax.sharding import PartitionSpec as P

MESH = pl.DeviceIdType.MESH
EXTRA = 16


def by_row(vector, rows):
    return jnp.transpose(jnp.broadcast_to(vector, (rows, vector.shape[1])))


def whiten_kernel(
    arcs, tile_map, lengths, amps, decays, design, obs, gaps, noise,
    white_t, live_m, noise_m, phi_m, amp_m, start_m, inno_m, var_m, parts,
):
    rows = design.shape[0]
    slots = design.shape[1] // rows
    row_tiles = (white_t.shape[1] - EXTRA) // rows
    live_row = gaps[...].astype(jnp.float32)
    live_m[...] = by_row(live_row, rows)
    noise_m[...] = by_row(noise[...], rows)
    position = lax.broadcasted_iota(jnp.int32, (rows, rows), 0)
    lane = lax.broadcasted_iota(jnp.int32, (rows, rows), 1)
    phi = jnp.zeros((rows, rows), jnp.float32)
    amp = jnp.zeros((rows, rows), jnp.float32)
    first = jnp.zeros((rows, rows), jnp.float32)
    begin = jnp.int32(0)
    for a in range(arcs):
        end = begin + lengths[0, a]
        inside = jnp.logical_and(position >= begin, position < end)
        phi = jnp.where(inside, decays[0, a], phi)
        amp = jnp.where(inside, amps[0, a], amp)
        first = jnp.where(jnp.logical_and(inside, position == begin), 1.0, first)
        begin = end
    phi_m[...] = jnp.where(first > 0.5, 0.0, phi)
    amp_m[...] = jnp.where(first > 0.5, amp, amp * (1.0 - phi * phi))
    start_m[...] = jnp.where(position == lane, 1.0, 0.0)

    def step(k, carry):
        state, spread = carry
        at = pl.ds(k, 1)
        rate, live, floor = phi_m[at, :], live_m[at, :], noise_m[at, :]
        state = rate * state
        spread = rate * rate * spread + amp_m[at, :]
        var = spread * live + floor
        ratio = 1.0 / var
        inno = live * (start_m[at, :] - state)
        inno_m[at, :] = inno
        var_m[at, :] = var
        return state + (spread * live * ratio) * inno, spread * floor * ratio

    zero = jnp.zeros((1, rows), jnp.float32)
    lax.fori_loop(0, rows, step, (zero, zero), unroll=8)
    inverse = inno_m[...] / jnp.sqrt(var_m[...])
    high = inverse.astype(jnp.bfloat16)
    rest = inverse - high.astype(jnp.float32)
    mid = rest.astype(jnp.bfloat16)
    parts[0] = high
    parts[1] = mid
    parts[2] = (rest - mid.astype(jnp.float32)).astype(jnp.bfloat16)

    def slot(s, _):
        column = pl.multiple_of(tile_map[s] * rows, rows)
        tile = design[:, pl.ds(column, rows)]
        solved = jnp.dot(parts[2], tile, preferred_element_type=jnp.float32)
        solved += jnp.dot(parts[1], tile, preferred_element_type=jnp.float32)
        solved += jnp.dot(parts[0], tile, preferred_element_type=jnp.float32)
        low = pl.multiple_of(lax.rem(s, row_tiles) * rows, rows)
        white_t[s // row_tiles, pl.ds(low, rows), :] = jnp.transpose(solved).astype(jnp.bfloat16)
        return 0

    lax.fori_loop(0, slots, slot, 0, unroll=4)
    obs_m = by_row(obs[...], rows)
    solved_obs = jnp.sum(jnp.transpose(inverse) * obs_m, axis=0, keepdims=True)
    o_high = solved_obs.astype(jnp.bfloat16).astype(jnp.float32)
    o_rest = solved_obs - o_high
    o_mid = o_rest.astype(jnp.bfloat16).astype(jnp.float32)
    which = lax.broadcasted_iota(jnp.int32, (EXTRA, rows), 0)
    packed = jnp.where(which == 0, o_high, 0.0)
    packed = jnp.where(which == 1, o_mid, packed)
    packed = jnp.where(which == 2, o_rest - o_mid, packed).astype(jnp.bfloat16)
    for r in range(white_t.shape[0]):
        white_t[r, row_tiles * rows :, :] = packed


def xor(a, b, limit):
    out, bit = 0, 1
    while bit < limit:
        out = out + bit * lax.rem(a // bit + b // bit, 2)
        bit *= 2
    return out


def gram_kernel(R, C, wt, gram, rhs, obs, rp, cp, *sems):
    (r1s, r1r, ups, upr, dns, dnr, chs, chr_, pas, par) = sems
    r, z = lax.axis_index("row"), lax.axis_index("col")
    M = gram.shape[0]
    G = R // 2
    core, chip = lax.rem(r, 2), r // 2

    def flip(mask):
        return xor(r, mask, R)

    zof = lambda d: lax.rem(z + (d % C), C)
    blk = lambda mask, d: flip(mask) * C + zof(d)
    apart = xor(chip, z, G)
    place, shift = apart, 2
    while shift <= G:
        place = xor(place, apart // shift, G)
        shift *= 2

    def seat(p):
        return 2 * xor(xor(p, p // 2, G), z, G) + core

    ahead = (seat(lax.rem(place + 1, G)), seat(lax.rem(place + G - 1, G)))
    steps = (place, lax.rem(G - place, G))

    barrier = pltpu.get_barrier_semaphore()
    for mask in range(1, R):
        pl.semaphore_signal(barrier, inc=1, device_id=(flip(mask), z), device_id_type=MESH)
    for d in range(1, C):
        pl.semaphore_signal(barrier, inc=1, device_id=(r, zof(d)), device_id_type=MESH)
    pl.semaphore_wait(barrier, R - 1 + C - 1)

    sent = []

    def remote(src, dst, ss, rs, to):
        return pltpu.make_async_remote_copy(
            src_ref=src, dst_ref=dst, send_sem=ss, recv_sem=rs, device_id=to, device_id_type=MESH
        )

    def send(*args):
        copy = remote(*args)
        copy.start()
        sent.append(copy)

    def arrived(dst, ss, rs):
        remote(dst, dst, ss, rs, (r, z)).wait_recv()

    def reach(d):
        long, short = C // 2, C - 1 - C // 2
        return (long, short) if d % 2 == 0 else (short, long)

    def ring(d, hop, way):
        at = blk(d, -hop if way > 0 else hop)
        src = wt.at[r] if d == 0 and hop == 0 else rp.at[at]
        ss, rs = (ups, upr) if way > 0 else (dns, dnr)
        send(src, rp.at[at], ss.at[d, hop], rs.at[d, hop], (r, zof(way)))

    def block_of(h, mask, dz):
        return xor(2 * z + h, mask, R) * C + zof(dz)

    def chain(src, mask, dz):
        at = block_of(core, mask, dz)
        return remote(
            src, cp.at[core, at], chs.at[mask, dz], chr_.at[mask, dz], (ahead[mask % 2], z)
        )

    def partner(src, mask, dz):
        at = block_of(core, mask, dz)
        return remote(src, cp.at[core, at], pas.at[mask, dz], par.at[mask, dz], (flip(1), z))

    def take(mask, dz):
        at = blk(mask, dz)
        if dz == 0:
            if mask:
                arrived(rp.at[at], r1s.at[mask], r1r.at[mask])
            up, down = reach(mask)
            if up > 0:
                ring(mask, 0, 1)
            if down > 0:
                ring(mask, 0, -1)
        else:
            up, down = reach(mask)
            if dz <= down:
                hop, way, last, ss, rs = dz - 1, -1, down, dns, dnr
            else:
                hop, way, last, ss, rs = C - dz - 1, 1, up, ups, upr
            arrived(rp.at[at], ss.at[mask, hop], rs.at[mask, hop])
            if hop + 1 < last:
                ring(mask, hop + 1, way)

        @pl.when(place == 0)
        def _():
            src = wt.at[r, :M] if mask == 0 and dz == 0 else rp.at[at, :M]
            chain(src, mask, dz).start()
            partner(src, mask, dz).start()
            cp[core, at] = rp[at, :M, :]

    def relay(mask, dz):
        at = block_of(core, mask, dz)

        @pl.when(place > 0)
        def _():
            src = cp.at[core, at]
            arrived(src, chs.at[mask, dz], chr_.at[mask, dz])

            @pl.when(steps[mask % 2] < G - 1)
            def _():
                chain(src, mask, dz).start()

            partner(src, mask, dz).start()

    K = rp.shape[2]
    wide = 256 if M % 256 == 0 else 128

    def accumulate(q, dz, fresh):
        b0 = 2 * q * C + zof(dz)
        b1 = b0 + C
        left = jnp.concatenate([rp[b0, :M, :], rp[b1, :M, :]], axis=1)
        seen = jnp.concatenate([rp[b0, M:, :], rp[b1, M:, :]], axis=1)
        obs[b0] = rp[b0, M:, :]
        obs[b1] = rp[b1, M:, :]
        nt = (((1,), (1,)), ((), ()))
        side = lax.dot_general(seen, left, nt, preferred_element_type=jnp.float32)
        if fresh:
            rhs[...] = side
        else:
            rhs[...] += side
        for h in (0, 1):

            def tile(j, _, h=h):
                at = pl.ds(pl.multiple_of(j * wide, wide), wide)
                to = pl.ds(pl.multiple_of(h * M + j * wide, wide), wide)
                lhs = jnp.concatenate([rp[b0, :M, :], rp[b1, :M, :]], axis=1)
                right = jnp.concatenate([cp[h, b0, at, :], cp[h, b1, at, :]], axis=1)
                part = lax.dot_general(lhs, right, nt, preferred_element_type=jnp.float32)
                if fresh:
                    gram[:, to] = part
                else:
                    gram[:, to] += part
                return 0

            lax.fori_loop(0, M // wide, tile, 0)

    masks = sorted(range(R), key=lambda m: (bin(m >> 1).count("1"), m))
    zs = sorted(range(C), key=lambda d: (min(d, C - d), d))
    for mask in masks[1:]:
        send(wt.at[flip(mask)], rp.at[r * C + z], r1s.at[mask], r1r.at[mask], (flip(mask), z))
    rp[r * C + z] = wt[r]
    items = [(mask, dz) for dz in zs for mask in masks]
    lag = 3
    for i in range(len(items) + lag):
        if i < len(items):
            take(*items[i])
        if i >= lag:
            j = i - lag
            relay(*items[j])
            phase, inside = divmod(j, R)
            if phase > 0 and inside % 2 == 1:
                if inside == 1:
                    for mask in masks:
                        dz = zs[phase - 1]
                        at = block_of(1 - core, mask, dz)
                        arrived(cp.at[1 - core, at], pas.at[mask, dz], par.at[mask, dz])
                accumulate(inside // 2, zs[phase - 1], phase == 1 and inside == 1)
    dz = zs[-1]
    for mask in masks:
        at = block_of(1 - core, mask, dz)
        arrived(cp.at[1 - core, at], pas.at[mask, dz], par.at[mask, dz])
    for q in range(G):
        accumulate(q, dz, False)
    for mask, dz in items:
        src = cp.at[core, block_of(core, mask, dz)]
        partner(src, mask, dz).wait_send()

        @pl.when(steps[mask % 2] < G - 1)
        def _():
            chain(src, mask, dz).wait_send()

    for copy in sent:
        copy.wait_send()


def on_device(R, C, design, observations, gaps, noise_var, lengths, amps, decays, plan, tile_map):
    rows, columns = design.shape
    tiles = tile_map.shape[0]
    width = columns // C
    tall = columns // R
    blocks = R * C
    vm = pl.BlockSpec(memory_space=pltpu.VMEM)
    sm = pl.BlockSpec(memory_space=pltpu.SMEM)
    square = pltpu.VMEM((rows, rows), jnp.float32)
    wt = pl.pallas_call(
        functools.partial(whiten_kernel, lengths.shape[1]),
        out_shape=jax.ShapeDtypeStruct((R, tall + EXTRA, rows), jnp.bfloat16),
        in_specs=[sm, sm, sm, sm, vm, vm, vm, vm],
        out_specs=vm,
        scratch_shapes=[square] * 7 + [pltpu.VMEM((3, rows, rows), jnp.bfloat16)],
        name="whiten",
    )(
        tile_map, lengths, amps, decays, design,
        observations[None, :], gaps[None, :], noise_var[None, :],
    )
    dma = lambda *shape: pltpu.SemaphoreType.DMA(shape)
    sems = []
    for shape in ((R,), (R, C), (R, C), (R, C), (R, C)):
        sems += [dma(*shape), dma(*shape)]
    gram, rhs, obs = pl.pallas_call(
        functools.partial(gram_kernel, R, C),
        out_shape=(
            jax.ShapeDtypeStruct((tall, width), jnp.float32),
            jax.ShapeDtypeStruct((EXTRA, tall), jnp.float32),
            jax.ShapeDtypeStruct((blocks, EXTRA, rows), jnp.bfloat16),
        ),
        in_specs=[vm],
        out_specs=(vm, vm, vm),
        scratch_shapes=[
            pltpu.VMEM((blocks, tall + EXTRA, rows), jnp.bfloat16),
            pltpu.VMEM((2, blocks, tall, rows), jnp.bfloat16),
        ]
        + sems,
        compiler_params=pltpu.CompilerParams(
            collective_id=0, has_side_effects=True, vmem_limit_bytes=63 * 1024 * 1024
        ),
        name="gram",
    )(wt)
    picked = jnp.take(obs, plan, axis=0).astype(jnp.float32)
    balanced = picked[:, 0] + (picked[:, 1] + picked[:, 2])
    return gram, rhs[0], balanced


def solution(mesh):
    both = ("row", "col")
    placed = (
        P(both, None), P(both), P(both), P(both), P(both, None), P(both, None), P(both, None),
        P(both), P(),
    )
    return jax.shard_map(
        functools.partial(on_device, mesh.shape["row"], mesh.shape["col"]),
        mesh=mesh,
        in_specs=placed,
        out_specs=(P("row", "col"), P("row"), P(both, None)),
        check_vma=False,
    )
```
